32 devices in a mesh: samp: 8 (over z, y), snp: 4 (over x, core).
Axes of the slice: x: 2, y: 2, z: 4, core: 2. Of those that a mesh axis runs over, the one named last changes fastest.
Arguments:
- geno_words: int32 [2048, 1024], P('samp', 'snp'), may hold values from -2147483648 to 2147483647, as said below
- counts: int32 [2048], P('samp'), may hold values from 0 to 4, as said below
- probes: bfloat16 [2048, 64], P('samp'), may hold values from -6 to 6
- phenotype: float32 [2048], P('samp'), may hold values from -6 to 6
- tile_comp: int32 [128], replicated, may hold values from 0 to 7, as said below
Outputs:
- images: bfloat16 [2048, 512], P(('samp', 'snp'))
- traces: float32 [8, 8], replicated
- yky: float32 [8], replicated
The draws below stay inside these ranges and needn't reach their ends.
Inputs may be any that keep to these rules, and one draw needn't show every extreme that they name: `geno_words`: each word packs sixteen dosages of one sample in 2-bit fields as step one reads them; every field holds 0, 1 or 2. `counts`: at least one sample has a count of one or more. `tile_comp`: every component owns at least one tile.
All inputs are finite; a program needn't handle non-finite values.
Results may differ from the reference program's by a relative error of at most 0.015.
Values may be sent and summed in bfloat16 or wider, within the bound.
A program may use at most 64 MiB of HBM per device.

```python
import math
import jax
import jax.numpy as jnp
from jax import lax

SNPS = 16384
PROBES = 64
COMPS = 8
NS = 2048
TILES = 128


def draw_geno_words(key, part):
    base = jax.random.randint(jax.random.fold_in(key, 11), (SNPS,), 51, 165)
    stride = math.gcd(NS, 512)
    shifts = 2 * jnp.arange(16, dtype=jnp.int32).reshape(1, 1, 16, 1)
    block_key = jax.random.fold_in(key, 12)

    def one_block(first_row):
        sample_ids = first_row + jnp.arange(stride, dtype=jnp.int32)
        levels = base[None, :] * (NS + 2 * sample_ids[:, None]) // NS
        drawn = jax.random.randint(jax.random.fold_in(block_key, first_row), (stride, SNPS), 0, 1048576)
        dosage = (drawn % 1024 < levels).astype(jnp.int32) + (drawn // 1024 < levels).astype(jnp.int32)
        fields = jnp.left_shift(dosage.reshape(stride, SNPS // 2048, 16, 128), shifts)
        return jnp.sum(fields, axis=2).reshape(stride, SNPS // 16)
    starts = jnp.arange(NS // stride, dtype=jnp.int32) * stride
    return lax.map(one_block, starts).reshape(NS, SNPS // 16)


def draw_counts(key, part):
    drawn = jax.random.randint(jax.random.fold_in(key, 21), (NS,), 0, 5)
    chosen = jax.random.randint(jax.random.fold_in(key, 22), (), 0, NS)
    return drawn.at[chosen].set(jnp.maximum(drawn[chosen], 1))


def draw_tile_comp(key, part):
    drawn = jax.random.randint(jax.random.fold_in(key, 31), (TILES,), 0, COMPS)
    shuffled = jax.random.permutation(jax.random.fold_in(key, 32), TILES)
    return drawn.at[shuffled[:COMPS]].set(jnp.arange(COMPS, dtype=jnp.int32))


def steps_of(own_key, extent, pieces, low, largest):
    gain, own = 1.0, jax.random.fold_in(own_key, 6)
    for position, shards_of in pieces:
        heights = jnp.exp(jax.random.uniform(jax.random.fold_in(own, position), (shards_of,), jnp.float32, low / len(pieces), largest / len(pieces)))
        gain = gain * jnp.repeat(heights, extent[position] // shards_of).reshape([-1 if axis == position else 1 for axis in range(len(extent))])
    return gain


def gaussian(key, extent, width, bound, pieces=(), held_as=jnp.bfloat16):
    values = width * jax.random.normal(key, extent, jnp.float32)
    if pieces:
        values = values * steps_of(key, extent, pieces, -0.22, 0.18)
    return jnp.clip(values, -bound, bound).astype(held_as)


def setup_inputs(seed: int = 0) -> dict:
    splits = jax.random.split(jax.random.key(seed), 6)
    return {
        "geno_words": draw_geno_words(jax.random.fold_in(splits[5], 71), 0),
        "counts": draw_counts(jax.random.fold_in(splits[5], 71), 0),
        "probes": gaussian(splits[2], (NS, PROBES), 1.0, 6.0, ((0, 8),)),
        "phenotype": gaussian(splits[3], (NS,), 1.0, 6.0, ((0, 8),), jnp.float32),
        "tile_comp": draw_tile_comp(jax.random.fold_in(splits[5], 71), 0),
    }


EPSILON = 1e-05

def unpack_rows(packed):
    height = packed.shape[0]
    grouped = packed.reshape(height, -1, 1, 128)
    shifts = 2 * jnp.arange(16, dtype=jnp.int32).reshape(1, 1, 16, 1)
    fields = jnp.right_shift(grouped, shifts) & 3
    return fields.reshape(height, -1).astype(jnp.bfloat16)

def reference(geno_words, counts, probes, phenotype, tile_comp):
    weights = counts.astype(jnp.float32)
    root_weight = jnp.sqrt(weights)
    probe_rows = (probes.astype(jnp.float32) * root_weight[:, None]).astype(jnp.bfloat16)
    pheno_rows = (phenotype * root_weight).astype(jnp.bfloat16)
    count_rows = counts.astype(jnp.bfloat16)
    stride = math.gcd(NS, 1024)
    blocks = NS // stride
    packed_blocks = geno_words.reshape(blocks, stride, SNPS // 16)

    def first_pass(running, inputs):
        cross_panel, moments = running
        packed, probe_block, pheno_block, count_block = inputs
        dosage = unpack_rows(packed)
        cross_panel = cross_panel + jnp.dot(dosage.T, probe_block, preferred_element_type=jnp.float32)
        increment = jnp.stack([jnp.dot(count_block, dosage, preferred_element_type=jnp.float32), jnp.dot(count_block, dosage * dosage, preferred_element_type=jnp.float32), jnp.dot(pheno_block, dosage, preferred_element_type=jnp.float32)])
        return ((cross_panel, moments + increment), None)
    start_pair = (jnp.zeros((SNPS, PROBES), jnp.float32), jnp.zeros((3, SNPS), jnp.float32))
    (cross_panel, moments), ignored = lax.scan(first_pass, start_pair, (packed_blocks, probe_rows.reshape(blocks, stride, PROBES), pheno_rows.reshape(blocks, stride), count_rows.reshape(blocks, stride)))
    weight_total = jnp.sum(weights)
    pheno_total = jnp.sum(pheno_rows.astype(jnp.float32))
    probe_total = lax.optimization_barrier(jnp.sum(probe_rows.astype(jnp.float32), axis=0))
    average = moments[0] / weight_total
    second = moments[1] / weight_total
    spread = 1.0 / jnp.sqrt(second - average * average + EPSILON)
    unit_panel = spread[:, None] * (cross_panel - average[:, None] * probe_total[None, :])
    pheno_unit = spread * (moments[2] - average * pheno_total)
    levels = jnp.arange(COMPS, dtype=jnp.int32)
    member_tiles = (tile_comp[:, None] == levels[None, :]).astype(jnp.float32)
    comp_sizes = 128.0 * lax.optimization_barrier(jnp.sum(member_tiles, axis=0))
    member_snps = jnp.repeat(member_tiles, 128, axis=0)
    inverse = lax.optimization_barrier(jnp.sum(member_snps * (1.0 / comp_sizes)[None, :], axis=1))
    coefficients = (spread[:, None] * unit_panel * inverse[:, None]).astype(jnp.bfloat16)
    energy = lax.optimization_barrier(jnp.sum(member_snps * (pheno_unit * pheno_unit * inverse)[:, None], axis=0))
    coef_tiles = coefficients.reshape(TILES, 128, PROBES).astype(jnp.float32)
    centre = lax.optimization_barrier(jnp.sum(average.reshape(TILES, 128, 1) * coef_tiles, axis=1))

    def second_pass(running, inputs):
        packed, root_block = inputs
        dosage = unpack_rows(packed).astype(jnp.float32).reshape(stride, TILES, 128)
        partial_value = jnp.einsum('rtj,tjb->rtb', dosage, coef_tiles, precision=lax.Precision.HIGHEST) - centre[None]
        grouped = jnp.einsum('rtb,tk->rkb', partial_value, member_tiles, precision=lax.Precision.HIGHEST)
        grouped = grouped * root_block[:, None, None]
        running = running + jnp.einsum('rkb,rlb->kl', grouped, grouped, precision=lax.Precision.HIGHEST)
        return (running, grouped.reshape(stride, COMPS * PROBES).astype(jnp.bfloat16))
    trace_sum, images = lax.scan(second_pass, jnp.zeros((COMPS, COMPS), jnp.float32), (packed_blocks, root_weight.reshape(blocks, stride)))
    traces = trace_sum * (SNPS / (COMPS * PROBES)) / (weight_total * weight_total)
    return (images.reshape(NS, COMPS * PROBES), traces, energy / weight_total)
```

```python
import functools
import jax
import jax.numpy as jnp
from jax import lax
from jax.experimental import pallas as pl
from jax.experimental.pallas import tpu as pltpu
from jax.sharding import PartitionSpec as P

SNPS = 16384
COMPS = 8


EPSILON = 1e-05


def unpack_rows(packed):
    height = packed.shape[0]
    grouped = packed.reshape(height, -1, 1, 128)
    shifts = 2 * jnp.arange(16, dtype=jnp.int32).reshape(1, 1, 16, 1)
    fields = jnp.right_shift(grouped, shifts) & 3
    return fields.reshape(height, -1).astype(jnp.bfloat16)


def block_number(row_count):
    number = 1
    while row_count // number > 768 or row_count % number != 0:
        number = number + 1
    return number


def finish(panel_part, moment_part, totals, inverse, member):
    weight_total = totals[0]
    pheno_total = totals[1]
    probe_total = totals[2:]
    average = moment_part[0] / weight_total
    second = moment_part[1] / weight_total
    spread = 1.0 / jnp.sqrt(second - average * average + EPSILON)
    unit_panel = spread[:, None] * (panel_part - average[:, None] * probe_total[None, :])
    pheno_unit = spread * (moment_part[2] - average * pheno_total)
    coefficients = (spread[:, None] * unit_panel * inverse[:, None]).astype(jnp.bfloat16)
    energy = jnp.sum(member * (pheno_unit * pheno_unit * inverse)[:, None], axis=0)
    return (average, coefficients, energy)


def on_device(geno_words, counts, probes, phenotype, tile_comp):
    height = geno_words.shape[0]
    snp_local = geno_words.shape[1] * 16
    tile_local = snp_local // 128
    probe_count = probes.shape[1]
    weights = counts.astype(jnp.float32)
    root_weight = jnp.sqrt(weights)
    probe_rows = (probes.astype(jnp.float32) * root_weight[:, None]).astype(jnp.bfloat16)
    pheno_rows = (phenotype * root_weight).astype(jnp.bfloat16)
    count_rows = counts.astype(jnp.bfloat16)
    left_rows = jnp.stack([count_rows, pheno_rows], axis=1)
    dosage = unpack_rows(geno_words)
    cross_panel = jnp.einsum("rj,rb->jb", dosage, probe_rows, preferred_element_type=jnp.float32)
    linear = jnp.einsum("rc,rj->cj", left_rows, dosage, preferred_element_type=jnp.float32)
    squares = jnp.einsum("r,rj->j", count_rows, dosage * dosage, preferred_element_type=jnp.float32)
    moments = jnp.stack([linear[0], squares, linear[1]])
    totals = jnp.concatenate(
        [
            jnp.sum(weights)[None],
            jnp.sum(pheno_rows.astype(jnp.float32))[None],
            jnp.sum(probe_rows.astype(jnp.float32), axis=0),
        ]
    )
    levels = jnp.arange(COMPS, dtype=jnp.int32)
    member_all = (tile_comp[:, None] == levels[None, :]).astype(jnp.float32)
    comp_sizes = 128.0 * jnp.sum(member_all, axis=0)
    member_tiles = lax.dynamic_slice_in_dim(
        member_all, lax.axis_index("snp") * tile_local, tile_local, 0
    )
    member_snps = jnp.repeat(member_tiles, 128, axis=0)
    inverse = jnp.sum(member_snps * (1.0 / comp_sizes)[None, :], axis=1)
    summed_panel, summed_moments, totals = lax.psum(
        (cross_panel.reshape(-1, 128), moments, totals), "samp"
    )
    average, coefficients, energy = finish(
        summed_panel.reshape(snp_local, probe_count), summed_moments, totals, inverse, member_snps
    )
    energy = lax.psum(energy, "snp")
    coef_tiles = coefficients.reshape(tile_local, 128, probe_count)
    centre = jnp.sum(average.reshape(tile_local, 128, 1) * coef_tiles.astype(jnp.float32), axis=1)
    quarter = height // lax.axis_size("snp")
    inner_count = block_number(quarter * lax.axis_size("snp"))
    piece_rows = quarter * lax.axis_size("snp") // inner_count
    dosage = unpack_rows(geno_words)
    dosage = dosage.reshape(piece_rows, tile_local, 128)
    partial_value = (
        jnp.einsum("rtj,tjb->rtb", dosage, coef_tiles, preferred_element_type=jnp.float32)
        - centre[None]
    )
    grouped = jnp.einsum(
        "rtb,tk->rkb", partial_value, member_tiles, precision=lax.Precision.HIGHEST
    )
    scaled = grouped * root_weight[:, None, None]
    pieces = scaled.reshape(piece_rows, COMPS * probe_count)
    own_images = lax.psum_scatter(pieces, "snp", scatter_dimension=0, tiled=True)
    stacked = own_images.reshape(quarter, COMPS, probe_count)
    local_trace = jnp.einsum("rkb,rlb->kl", stacked, stacked, precision=lax.Precision.HIGHEST)
    trace_sum = lax.psum(local_trace, ("samp", "snp"))
    weight_total = totals[0]
    traces = trace_sum * (SNPS / (COMPS * probe_count)) / (weight_total * weight_total)
    return (own_images.astype(jnp.bfloat16), traces, energy / weight_total)


MESH = pl.DeviceIdType.MESH
HIGHEST = lax.Precision.HIGHEST


def whole_kernel(
    sizes,
    tile_smem,
    words_ref,
    counts_ref,
    probes_ref,
    pheno_ref,
    tile_ref,
    images_ref,
    traces_ref,
    yky_ref,
    dosage,
    panel_out,
    moment_out,
    panel_in,
    moment_in,
    coef,
    spread_coef,
    total,
    piece_out,
    piece_in,
    sum_samp,
    sum_snp,
    sum_mid,
    send_panel,
    recv_panel,
    send_moment,
    recv_moment,
    send_coef,
    recv_coef,
    send_piece,
    recv_piece,
    send_samp,
    recv_samp,
    send_snp,
    recv_snp,
):
    n_samp, n_snp, tiles_local, probe_count = sizes
    me, mine = lax.axis_index("samp"), lax.axis_index("snp")
    chunk_tiles = tiles_local // n_samp
    width = chunk_tiles * 128
    height = words_ref.shape[0]
    rows = height // n_snp
    panel_rows = probe_count
    f32, bf16 = jnp.float32, jnp.bfloat16

    def samp_peer(offset):
        return lax.rem(me + offset, n_samp)

    def snp_peer(offset):
        return lax.rem(mine + offset, n_snp)

    barrier = pltpu.get_barrier_semaphore()
    for o in range(1, n_samp):
        pl.semaphore_signal(barrier, inc=1, device_id={"samp": samp_peer(o)}, device_id_type=MESH)
    for o in range(1, n_snp):
        pl.semaphore_signal(barrier, inc=1, device_id={"snp": snp_peer(o)}, device_id_type=MESH)

    def remote(src, dst, send, recv, axis, peer):
        return pltpu.make_async_remote_copy(
            src_ref=src, dst_ref=dst, send_sem=send, recv_sem=recv,
            device_id={axis: peer}, device_id_type=MESH,
        )

    weights = counts_ref[...].astype(f32)
    root = jnp.sqrt(weights)
    probe_t = probes_ref[...].astype(f32).T
    probe_rows = (probe_t * root).astype(bf16)
    pheno_rows = (pheno_ref[...] * root).astype(bf16)
    low = lax.broadcasted_iota(jnp.int32, (16, height), 0)
    extra = jnp.where(
        low == 0, weights, jnp.where(low == 1, pheno_rows.astype(f32), 0.0)
    ).astype(bf16)
    left = jnp.concatenate([probe_rows, extra], axis=0)
    count_left = jnp.where(low == 0, weights, 0.0).astype(bf16)

    own_sums = jnp.sum(left.astype(f32), axis=1, keepdims=True)
    own_column = own_sums[:panel_rows]
    own_weight = own_sums[panel_rows:panel_rows + 1]
    padded = jnp.concatenate(
        [
            jnp.broadcast_to(own_sums, (panel_rows + 16, 128)),
            jnp.zeros((128 - panel_rows - 16, 128), f32),
        ],
        axis=0,
    )
    own_row = padded.T[0:1]
    own_row_wide = jnp.concatenate([own_row] * chunk_tiles, axis=1)
    own_scale = 1.0 / jnp.maximum(own_weight, 1.0)

    own_panel = None
    own_moment = None
    order = list(range(1, n_samp)) + [0]
    for step, o in enumerate(order):
        owner = samp_peer(o)
        pieces = []
        for tt in range(chunk_tiles):
            tile = owner * chunk_tiles + tt
            group = lax.div(tile, 16)
            shift = 2 * lax.rem(tile, 16)
            words = words_ref[:, pl.ds(pl.multiple_of(group * 128, 128), 128)]
            pieces.append((lax.shift_right_logical(words, jnp.broadcast_to(shift, words.shape)) & 3).astype(f32).astype(bf16))
        x = jnp.concatenate(pieces, axis=1)
        dosage[o, :height, :] = x
        linear = jnp.dot(left, x, preferred_element_type=f32)
        squares = jnp.dot(count_left, x * x, preferred_element_type=f32)
        first = linear[panel_rows:panel_rows + 1]
        panel = linear[:panel_rows] - own_column * (first * own_scale)
        moment = jnp.concatenate(
            [
                first,
                squares[0:1],
                linear[panel_rows + 1:panel_rows + 2],
                own_row_wide,
                jnp.zeros((4, width), f32),
            ],
            axis=0,
        )
        if o == 0:
            own_panel, own_moment = panel, moment
        else:
            panel_out[o] = panel.astype(bf16)
            moment_out[o] = moment
            if step == 0:
                pl.semaphore_wait(barrier, n_samp + n_snp - 2)
            remote(panel_out.at[o], panel_in.at[o], send_panel.at[o], recv_panel.at[o], "samp", owner).start()
            remote(moment_out.at[o], moment_in.at[o], send_moment.at[o], recv_moment.at[o], "samp", owner).start()

    root_wide = jnp.broadcast_to(root, (128, height)).T

    moments = [own_moment]
    panel_sum = own_panel
    for o in range(1, n_samp):
        remote(moment_out.at[o], moment_in.at[o], send_moment.at[o], recv_moment.at[o], "samp", samp_peer(o)).wait_recv()
        remote(panel_out.at[o], panel_in.at[o], send_panel.at[o], recv_panel.at[o], "samp", samp_peer(o)).wait_recv()
        moments.append(moment_in[o])
        panel_sum = panel_sum + panel_in[o].astype(f32)
    moment_sum = moments[0]
    for item in moments[1:]:
        moment_sum = moment_sum + item
    row_stack = jnp.concatenate(
        [item[3:4, :128] for item in moments] + [jnp.zeros((128 - n_samp, 128), f32)], axis=0
    )
    columns = row_stack.T
    totals = jnp.sum(columns, axis=1, keepdims=True)
    weight_total = totals[panel_rows:panel_rows + 1]
    pheno_total = totals[panel_rows + 1:panel_rows + 2]
    average = moment_sum[0:1] / weight_total
    second = moment_sum[1:2] / weight_total
    spread = 1.0 / jnp.sqrt(second - average * average + EPSILON)
    shifts = []
    for index, item in enumerate(moments):
        own = columns[panel_rows:panel_rows + 1, index:index + 1]
        shifts.append(item[0:1] * (1.0 / jnp.maximum(own, 1.0)) - average)
    shifts.append(jnp.zeros((128 - n_samp, width), f32))
    correction = jnp.dot(
        columns[:panel_rows], jnp.concatenate(shifts, axis=0),
        precision=HIGHEST, preferred_element_type=f32,
    )
    unit_panel = spread * (panel_sum + correction)
    pheno_unit = spread * (moment_sum[2:3] - average * pheno_total)

    tile_all = tile_ref[...]
    inverse_parts = []
    lanes = lax.broadcasted_iota(jnp.int32, (1, 128), 1)
    tile_first = mine * tiles_local
    own_tiles = [tile_smem[tile_first + me * chunk_tiles + tt] for tt in range(chunk_tiles)]
    for tt in range(chunk_tiles):
        size = 128.0 * jnp.sum((tile_all == own_tiles[tt]).astype(f32), axis=1, keepdims=True)
        inverse_parts.append(jnp.broadcast_to(1.0 / size, (1, 128)))
    inverse = jnp.concatenate(inverse_parts, axis=1)
    coefficients = (spread * unit_panel * inverse).astype(bf16)
    high = average.astype(bf16).astype(f32)
    rest = average - high
    middle = rest.astype(bf16).astype(f32)
    last = rest - middle
    low_wide = lax.broadcasted_iota(jnp.int32, (16, width), 0)
    average_rows = jnp.where(
        low_wide == 0, high, jnp.where(low_wide == 1, middle, jnp.where(low_wide == 2, last, 0.0))
    ).astype(bf16)
    coef[0, :panel_rows, :] = coefficients
    coef[0, panel_rows:, :] = average_rows
    for o in range(1, n_samp):
        remote(coef.at[0], coef.at[n_samp - o], send_coef.at[o], recv_coef.at[n_samp - o], "samp", samp_peer(o)).start()

    energy_snps = pheno_unit * pheno_unit * inverse
    energy = jnp.zeros((1, 128), f32)
    for tt in range(chunk_tiles):
        part = jnp.sum(energy_snps[:, tt * 128:(tt + 1) * 128], axis=1, keepdims=True)
        energy = energy + jnp.where(lanes == own_tiles[tt], part, 0.0)

    wide_lane = lax.broadcasted_iota(jnp.int32, (1, width), 1)
    wait_order = [0]
    for o in range(1, n_samp // 2 + 1):
        wait_order.append(o)
        if n_samp - o != o:
            wait_order.append(n_samp - o)
    for step, s in enumerate(wait_order):
        owner = samp_peer(s)
        if s != 0:
            remote(coef.at[0], coef.at[s], send_coef.at[s], recv_coef.at[s], "samp", owner).wait_recv()
        comp = jnp.zeros((1, width), jnp.int32)
        for tt in range(chunk_tiles):
            number = tile_smem[tile_first + owner * chunk_tiles + tt]
            comp = jnp.where(lax.div(wide_lane, 128) == tt, number, comp)
        part = coef[s, :panel_rows, :]
        for k in range(COMPS):
            mask = (comp == k).astype(f32).astype(bf16)
            spread_coef[step % 2, k * panel_rows:(k + 1) * panel_rows, :] = part * mask
        dosage[s, height:, :] = coef[s, panel_rows:, :]
        product = lax.dot_general(
            dosage[s], spread_coef[step % 2], (((1,), (1,)), ((), ())), preferred_element_type=f32
        )
        if step == 0:
            total[...] = product
        else:
            total[...] += product

    centre = total[height:height + 1, :] + (total[height + 1:height + 2, :] + total[height + 2:height + 3, :])
    total[:height, :] = (total[:height, :] - centre) * jnp.concatenate(
        [root_wide] * (COMPS * probe_count // 128), axis=1
    )
    for o in range(1, n_snp):
        peer = snp_peer(o)
        piece_out[o] = total[pl.ds(pl.multiple_of(peer * rows, rows), rows), :].astype(bf16)
        remote(piece_out.at[o], piece_in.at[o], send_piece.at[o], recv_piece.at[o], "snp", peer).start()
    image = total[pl.ds(pl.multiple_of(mine * rows, rows), rows), :]
    for o in range(1, n_snp):
        remote(piece_out.at[o], piece_in.at[o], send_piece.at[o], recv_piece.at[o], "snp", snp_peer(o)).wait_recv()
        image = image + piece_in[o].astype(f32)
    images_ref[...] = image.astype(bf16)

    span = COMPS * probe_count
    turned = pltpu.roll(image, span - probe_count, 1)
    sums = []
    for d in range(COMPS):
        base = image if d % 2 == 0 else turned
        cut = (d // 2) * 2 * probe_count
        other = base if cut == 0 else jnp.concatenate([base[:, cut:], base[:, :cut]], axis=1)
        sums.append(jnp.sum(image * other, axis=0, keepdims=True))
    stacked = jnp.concatenate(sums, axis=0)
    picker = (
        lax.div(lax.broadcasted_iota(jnp.int32, (span, 128), 0), probe_count)
        == lax.broadcasted_iota(jnp.int32, (span, 128), 1)
    ).astype(f32)
    pairs = jnp.dot(stacked, picker, precision=HIGHEST, preferred_element_type=f32)

    sum_samp[me, 0:COMPS, :] = pairs
    sum_samp[me, COMPS:, :] = jnp.broadcast_to(energy, (8, 128))
    for o in range(1, n_samp):
        remote(sum_samp.at[me], sum_samp.at[me], send_samp.at[o], recv_samp.at[o], "samp", samp_peer(o)).start()
    for o in range(1, n_samp):
        source = lax.rem(me + n_samp - o, n_samp)
        remote(sum_samp.at[source], sum_samp.at[source], send_samp.at[o], recv_samp.at[o], "samp", samp_peer(o)).wait_recv()
    group_sum = sum_samp[0]
    for i in range(1, n_samp):
        group_sum = group_sum + sum_samp[i]
    sum_mid[...] = group_sum
    for o in range(1, n_snp):
        remote(sum_mid, sum_snp.at[mine], send_snp.at[o], recv_snp.at[o], "snp", snp_peer(o)).start()
    sum_snp[mine] = group_sum
    for o in range(1, n_snp):
        source = lax.rem(mine + n_snp - o, n_snp)
        remote(sum_mid, sum_snp.at[source], send_snp.at[o], recv_snp.at[o], "snp", snp_peer(o)).wait_recv()
    everything = sum_snp[0]
    for i in range(1, n_snp):
        everything = everything + sum_snp[i]
    row_id = lax.broadcasted_iota(jnp.int32, (COMPS, 128), 0)
    lane_id = lax.broadcasted_iota(jnp.int32, (COMPS, 128), 1)
    turn = (row_id - lane_id) & (COMPS - 1)
    trace = jnp.zeros((COMPS, 128), f32)
    for d in range(COMPS):
        trace = jnp.where(turn == d, everything[d:d + 1], trace)
    trace = trace * (SNPS / (COMPS * probe_count)) / (weight_total * weight_total)
    traces_ref[...] = trace[:, :COMPS]
    yky_ref[...] = (everything[COMPS:COMPS + 1] / weight_total)[:, :COMPS]

    for o in range(1, n_samp):
        remote(panel_out.at[o], panel_in.at[o], send_panel.at[o], recv_panel.at[o], "samp", samp_peer(o)).wait_send()
        remote(moment_out.at[o], moment_in.at[o], send_moment.at[o], recv_moment.at[o], "samp", samp_peer(o)).wait_send()
        remote(coef.at[0], coef.at[n_samp - o], send_coef.at[o], recv_coef.at[n_samp - o], "samp", samp_peer(o)).wait_send()
        remote(sum_samp.at[me], sum_samp.at[me], send_samp.at[o], recv_samp.at[o], "samp", samp_peer(o)).wait_send()
    for o in range(1, n_snp):
        remote(piece_out.at[o], piece_in.at[o], send_piece.at[o], recv_piece.at[o], "snp", snp_peer(o)).wait_send()
        remote(sum_mid, sum_snp.at[mine], send_snp.at[o], recv_snp.at[o], "snp", snp_peer(o)).wait_send()


def on_device_fused(geno_words, counts, probes, phenotype, tile_comp):
    n_samp, n_snp = lax.axis_size("samp"), lax.axis_size("snp")
    height = geno_words.shape[0]
    tiles_local = geno_words.shape[1] * 16 // 128
    probe_count = probes.shape[1]
    width = tiles_local // n_samp * 128
    span = COMPS * probe_count
    rows = height // n_snp
    f32, bf16 = jnp.float32, jnp.bfloat16
    vmem = pl.BlockSpec(memory_space=pltpu.VMEM)
    smem = pl.BlockSpec(memory_space=pltpu.SMEM)
    dma = pltpu.SemaphoreType.DMA
    images, traces, yky = pl.pallas_call(
        functools.partial(whole_kernel, (n_samp, n_snp, tiles_local, probe_count)),
        out_shape=(
            jax.ShapeDtypeStruct((rows, span), bf16),
            jax.ShapeDtypeStruct((COMPS, COMPS), f32),
            jax.ShapeDtypeStruct((1, COMPS), f32),
        ),
        in_specs=[smem] + [vmem] * 5,
        out_specs=(vmem, vmem, vmem),
        scratch_shapes=[
            pltpu.VMEM((n_samp, height + 16, width), bf16),
            pltpu.VMEM((n_samp, probe_count, width), bf16),
            pltpu.VMEM((n_samp, 8, width), f32),
            pltpu.VMEM((n_samp, probe_count, width), bf16),
            pltpu.VMEM((n_samp, 8, width), f32),
            pltpu.VMEM((n_samp, probe_count + 16, width), bf16),
            pltpu.VMEM((2, span, width), bf16),
            pltpu.VMEM((height + 16, span), f32),
            pltpu.VMEM((n_snp, rows, span), bf16),
            pltpu.VMEM((n_snp, rows, span), bf16),
            pltpu.VMEM((n_samp, COMPS + 8, 128), f32),
            pltpu.VMEM((n_snp, COMPS + 8, 128), f32),
            pltpu.VMEM((COMPS + 8, 128), f32),
            dma((n_samp,)),
            dma((n_samp,)),
            dma((n_samp,)),
            dma((n_samp,)),
            dma((n_samp,)),
            dma((n_samp,)),
            dma((n_snp,)),
            dma((n_snp,)),
            dma((n_samp,)),
            dma((n_samp,)),
            dma((n_snp,)),
            dma((n_snp,)),
        ],
        compiler_params=pltpu.CompilerParams(collective_id=0, has_side_effects=True),
    )(
        tile_comp,
        geno_words,
        counts.reshape(1, -1),
        probes,
        phenotype.reshape(1, -1),
        tile_comp.reshape(1, -1),
    )
    return (images, traces, yky.reshape(-1))


def dispatch(geno_words, counts, probes, phenotype, tile_comp):
    n_samp, n_snp = lax.axis_size("samp"), lax.axis_size("snp")
    tiles_local = geno_words.shape[1] * 16 // 128
    whole_tiles = tiles_local % n_samp == 0 and tile_comp.shape[0] == 128
    whole_rows = geno_words.shape[0] % (16 * n_snp) == 0 and probes.shape[1] == 64
    body = on_device_fused if whole_tiles and whole_rows else on_device
    return body(geno_words, counts, probes, phenotype, tile_comp)


def solution(mesh):
    in_specs = (P("samp", "snp"), P("samp"), P("samp", None), P("samp"), P())
    out_specs = (P(("samp", "snp"), None), P(), P())
    return jax.shard_map(
        dispatch, mesh=mesh, in_specs=in_specs, out_specs=out_specs, check_vma=False
    )
```

```python
import functools
import jax
import jax.numpy as jnp
from jax import lax
from jax.experimental import pallas as pl
from jax.experimental.pallas import tpu as pltpu
from jax.sharding import PartitionSpec as P

SNPS = 16384
COMPS = 8


EPSILON = 1e-05


def unpack_rows(packed):
    height = packed.shape[0]
    grouped = packed.reshape(height, -1, 1, 128)
    shifts = 2 * jnp.arange(16, dtype=jnp.int32).reshape(1, 1, 16, 1)
    fields = jnp.right_shift(grouped, shifts) & 3
    return fields.reshape(height, -1).astype(jnp.bfloat16)


def block_number(row_count):
    number = 1
    while row_count // number > 768 or row_count % number != 0:
        number = number + 1
    return number


def finish(panel_part, moment_part, totals, inverse, member):
    weight_total = totals[0]
    pheno_total = totals[1]
    probe_total = totals[2:]
    average = moment_part[0] / weight_total
    second = moment_part[1] / weight_total
    spread = 1.0 / jnp.sqrt(second - average * average + EPSILON)
    unit_panel = spread[:, None] * (panel_part - average[:, None] * probe_total[None, :])
    pheno_unit = spread * (moment_part[2] - average * pheno_total)
    coefficients = (spread[:, None] * unit_panel * inverse[:, None]).astype(jnp.bfloat16)
    energy = jnp.sum(member * (pheno_unit * pheno_unit * inverse)[:, None], axis=0)
    return (average, coefficients, energy)


def on_device(geno_words, counts, probes, phenotype, tile_comp):
    height = geno_words.shape[0]
    snp_local = geno_words.shape[1] * 16
    tile_local = snp_local // 128
    probe_count = probes.shape[1]
    weights = counts.astype(jnp.float32)
    root_weight = jnp.sqrt(weights)
    probe_rows = (probes.astype(jnp.float32) * root_weight[:, None]).astype(jnp.bfloat16)
    pheno_rows = (phenotype * root_weight).astype(jnp.bfloat16)
    count_rows = counts.astype(jnp.bfloat16)
    left_rows = jnp.stack([count_rows, pheno_rows], axis=1)
    dosage = unpack_rows(geno_words)
    cross_panel = jnp.einsum("rj,rb->jb", dosage, probe_rows, preferred_element_type=jnp.float32)
    linear = jnp.einsum("rc,rj->cj", left_rows, dosage, preferred_element_type=jnp.float32)
    squares = jnp.einsum("r,rj->j", count_rows, dosage * dosage, preferred_element_type=jnp.float32)
    moments = jnp.stack([linear[0], squares, linear[1]])
    totals = jnp.concatenate(
        [
            jnp.sum(weights)[None],
            jnp.sum(pheno_rows.astype(jnp.float32))[None],
            jnp.sum(probe_rows.astype(jnp.float32), axis=0),
        ]
    )
    levels = jnp.arange(COMPS, dtype=jnp.int32)
    member_all = (tile_comp[:, None] == levels[None, :]).astype(jnp.float32)
    comp_sizes = 128.0 * jnp.sum(member_all, axis=0)
    member_tiles = lax.dynamic_slice_in_dim(
        member_all, lax.axis_index("snp") * tile_local, tile_local, 0
    )
    member_snps = jnp.repeat(member_tiles, 128, axis=0)
    inverse = jnp.sum(member_snps * (1.0 / comp_sizes)[None, :], axis=1)
    summed_panel, summed_moments, totals = lax.psum(
        (cross_panel.reshape(-1, 128), moments, totals), "samp"
    )
    average, coefficients, energy = finish(
        summed_panel.reshape(snp_local, probe_count), summed_moments, totals, inverse, member_snps
    )
    energy = lax.psum(energy, "snp")
    coef_tiles = coefficients.reshape(tile_local, 128, probe_count)
    centre = jnp.sum(average.reshape(tile_local, 128, 1) * coef_tiles.astype(jnp.float32), axis=1)
    quarter = height // lax.axis_size("snp")
    inner_count = block_number(quarter * lax.axis_size("snp"))
    piece_rows = quarter * lax.axis_size("snp") // inner_count
    dosage = unpack_rows(geno_words)
    dosage = dosage.reshape(piece_rows, tile_local, 128)
    partial_value = (
        jnp.einsum("rtj,tjb->rtb", dosage, coef_tiles, preferred_element_type=jnp.float32)
        - centre[None]
    )
    grouped = jnp.einsum(
        "rtb,tk->rkb", partial_value, member_tiles, precision=lax.Precision.HIGHEST
    )
    scaled = grouped * root_weight[:, None, None]
    pieces = scaled.reshape(piece_rows, COMPS * probe_count)
    own_images = lax.psum_scatter(pieces, "snp", scatter_dimension=0, tiled=True)
    stacked = own_images.reshape(quarter, COMPS, probe_count)
    local_trace = jnp.einsum("rkb,rlb->kl", stacked, stacked, precision=lax.Precision.HIGHEST)
    trace_sum = lax.psum(local_trace, ("samp", "snp"))
    weight_total = totals[0]
    traces = trace_sum * (SNPS / (COMPS * probe_count)) / (weight_total * weight_total)
    return (own_images.astype(jnp.bfloat16), traces, energy / weight_total)


MESH = pl.DeviceIdType.MESH
HIGHEST = lax.Precision.HIGHEST
HALVES = 2
PAIR = 2


def whole_kernel(
    sizes,
    tile_smem,
    words_ref,
    counts_ref,
    probes_ref,
    pheno_ref,
    tile_ref,
    images_ref,
    traces_ref,
    yky_ref,
    dosage,
    keep,
    pair_out,
    pair_note_out,
    pair_in,
    pair_note_in,
    line_out,
    line_note_out,
    line_in,
    line_note_in,
    coef,
    means,
    spread_coef,
    total,
    piece_out,
    piece_in,
    sum_samp,
    sum_snp,
    sum_mid,
    send_pair,
    recv_pair,
    send_pair_note,
    recv_pair_note,
    send_line,
    recv_line,
    send_line_note,
    recv_line_note,
    send_coef,
    recv_coef,
    send_means,
    recv_means,
    send_piece,
    recv_piece,
    send_samp,
    recv_samp,
    send_snp,
    recv_snp,
):
    n_samp, n_snp, tiles_local, probe_count, halves = sizes
    me, mine = lax.axis_index("samp"), lax.axis_index("snp")
    n_line = n_samp // PAIR
    line, side = lax.div(me, PAIR), lax.rem(me, PAIR)
    partner = line * PAIR + (1 - side)
    chunk_tiles = tiles_local // n_samp
    block_tiles = chunk_tiles // halves
    width = block_tiles * 128
    note_rows = pair_note_in.shape[2]
    height = words_ref.shape[0]
    rows = height // n_snp
    panel_rows = probe_count
    f32, bf16 = jnp.float32, jnp.bfloat16

    def samp_peer(offset):
        return lax.rem(me + offset, n_samp)

    def snp_peer(offset):
        return lax.rem(mine + offset, n_snp)

    def line_peer(offset):
        return lax.rem(line + offset, n_line) * PAIR + side

    def owner_of(offset, other):
        return lax.rem(line + offset, n_line) * PAIR + (1 - side if other else side)

    far_first = sorted(range(1, n_line), key=lambda o: -min(o, n_line - o))
    near_first = sorted(range(1, n_line), key=lambda o: min(o, n_line - o))

    barrier = pltpu.get_barrier_semaphore()
    for o in range(1, n_samp):
        pl.semaphore_signal(barrier, inc=1, device_id={"samp": samp_peer(o)}, device_id_type=MESH)
    for o in range(1, n_snp):
        pl.semaphore_signal(barrier, inc=1, device_id={"snp": snp_peer(o)}, device_id_type=MESH)

    def remote(src, dst, send, recv, axis, peer):
        return pltpu.make_async_remote_copy(
            src_ref=src, dst_ref=dst, send_sem=send, recv_sem=recv,
            device_id={axis: peer}, device_id_type=MESH,
        )

    def pair_copies(h, o):
        return (
            remote(pair_out.at[h, o], pair_in.at[h, o], send_pair.at[h, o], recv_pair.at[h, o], "samp", partner),
            remote(pair_note_out.at[h, o], pair_note_in.at[h, o], send_pair_note.at[h, o], recv_pair_note.at[h, o], "samp", partner),
        )

    def line_copies(h, o):
        return (
            remote(line_out.at[h, o], line_in.at[h, o], send_line.at[h, o], recv_line.at[h, o], "samp", line_peer(o)),
            remote(line_note_out.at[h, o], line_note_in.at[h, o], send_line_note.at[h, o], recv_line_note.at[h, o], "samp", line_peer(o)),
        )

    def coef_copies(h, source, target, send, peer):
        return (
            remote(coef.at[h, source], coef.at[h, target], send_coef.at[h, send], recv_coef.at[h, target], "samp", peer),
            remote(means.at[h, source], means.at[h, target], send_means.at[h, send], recv_means.at[h, target], "samp", peer),
        )

    def start(copies):
        for item in copies:
            item.start()

    def received(copies):
        for item in copies:
            item.wait_recv()

    def note_of(first, second, third, last):
        parts = [v[:, t * 128:(t + 1) * 128] for v in (first, second, third) for t in range(block_tiles)]
        parts.append(last)
        spare = note_rows - len(parts)
        if spare:
            parts.append(jnp.zeros((spare, 128), f32))
        return jnp.concatenate(parts, axis=0)

    def wide_of(note, row):
        return jnp.concatenate([note[row * block_tiles + t:row * block_tiles + t + 1] for t in range(block_tiles)], axis=1)

    def last_of(note):
        return note[3 * block_tiles:3 * block_tiles + 1]

    weights = counts_ref[...].astype(f32)
    root = jnp.sqrt(weights)
    probe_rows = (probes_ref[...].astype(f32) * root).astype(bf16)
    pheno_rows = (pheno_ref[...] * root).astype(bf16)
    low = lax.broadcasted_iota(jnp.int32, (16, height), 0)
    extra = jnp.where(
        low == 0, weights, jnp.where(low == 1, pheno_rows.astype(f32), 0.0)
    ).astype(bf16)
    left = jnp.concatenate([probe_rows, extra], axis=0)
    count_left = jnp.where(low == 0, weights, 0.0).astype(bf16)

    own_sums = jnp.sum(left.astype(f32), axis=1, keepdims=True)
    own_column = own_sums[:panel_rows]
    own_weight = own_sums[panel_rows:panel_rows + 1]
    padded = jnp.concatenate(
        [
            jnp.broadcast_to(own_sums, (panel_rows + 16, 128)),
            jnp.zeros((128 - panel_rows - 16, 128), f32),
        ],
        axis=0,
    )
    own_row = padded.T[0:1]
    own_scale = 1.0 / jnp.maximum(own_weight, 1.0)

    def block(h, o, other):
        owner = owner_of(o, other)
        pieces = []
        for tt in range(block_tiles):
            tile = owner * chunk_tiles + h * block_tiles + tt
            group = lax.div(tile, 16)
            shift = 2 * lax.rem(tile, 16)
            words = words_ref[:, pl.ds(pl.multiple_of(group * 128, 128), 128)]
            field = lax.shift_right_logical(words, jnp.broadcast_to(shift, words.shape)) & 3
            pieces.append(field.astype(f32).astype(bf16))
        x = jnp.concatenate(pieces, axis=1)
        dosage[h, o * PAIR + other, :height, :] = x
        linear = jnp.dot(left, x, preferred_element_type=f32)
        squares = jnp.dot(count_left, x * x, preferred_element_type=f32)
        first = linear[panel_rows:panel_rows + 1]
        middle = first * own_scale
        panel = linear[:panel_rows] - own_column * middle
        return panel, first, squares[0:1], linear[panel_rows + 1:panel_rows + 2], middle

    waited = False
    for h in range(halves):
        for o in far_first + [0]:
            panel, first, square, cross, middle = block(h, o, 1)
            pair_out[h, o] = panel.astype(bf16)
            pair_note_out[h, o] = note_of(first, square, cross, own_row)
            if not waited:
                pl.semaphore_wait(barrier, n_samp + n_snp - 2)
                waited = True
            start(pair_copies(h, o))
    own_notes = {}
    for h in range(halves):
        for o in far_first + [0]:
            panel, first, square, cross, middle = block(h, o, 0)
            keep[h, o] = panel
            own_notes[h, o] = (first, square, cross, middle)
    root_wide = jnp.broadcast_to(root, (128, height)).T

    other_column = None
    own_pair = {}
    for h in range(halves):
        for o in far_first + [0]:
            received(pair_copies(h, o))
            note = pair_note_in[h, o]
            if other_column is None:
                other_row = last_of(note)
                turned = jnp.broadcast_to(other_row, (128, 128)).T[:, 0:1]
                other_column = turned[:panel_rows]
                other_weight = turned[panel_rows:panel_rows + 1]
                other_scale = 1.0 / jnp.maximum(other_weight, 1.0)
                pair_scale = 1.0 / jnp.maximum(own_weight + other_weight, 1.0)
                pair_row = own_row + other_row
            first, square, cross, middle = own_notes[h, o]
            other_first = wide_of(note, 0)
            pair_first = first + other_first
            pair_middle = pair_first * pair_scale
            panel = (
                keep[h, o]
                + pair_in[h, o].astype(f32)
                + own_column * (middle - pair_middle)
                + other_column * (other_first * other_scale - pair_middle)
            )
            pair_note = (pair_first, square + wide_of(note, 1), cross + wide_of(note, 2))
            if o == 0:
                own_pair[h] = (panel, pair_note)
            else:
                line_out[h, o] = panel.astype(bf16)
                line_note_out[h, o] = note_of(*pair_note, pair_row)
                start(line_copies(h, o))

    tile_all = tile_ref[...]
    lanes = lax.broadcasted_iota(jnp.int32, (1, 128), 1)
    tile_first = mine * tiles_local
    own_tiles = [tile_smem[tile_first + me * chunk_tiles + tt] for tt in range(chunk_tiles)]
    inverse_parts = []
    for tt in range(chunk_tiles):
        size = 128.0 * jnp.sum((tile_all == own_tiles[tt]).astype(f32), axis=1, keepdims=True)
        inverse_parts.append(jnp.broadcast_to(1.0 / size, (1, 128)))

    columns = None
    energy = jnp.zeros((1, 128), f32)
    for h in range(halves):
        panel_sum, own_note = own_pair[h]
        notes = [own_note]
        last_rows = [pair_row]
        for o in far_first:
            received(line_copies(h, o))
            note = line_note_in[h, o]
            panel_sum = panel_sum + line_in[h, o].astype(f32)
            notes.append((wide_of(note, 0), wide_of(note, 1), wide_of(note, 2)))
            last_rows.append(last_of(note))
        if columns is None:
            columns = jnp.concatenate(last_rows + [jnp.zeros((128 - n_line, 128), f32)], axis=0).T
            totals = jnp.sum(columns, axis=1, keepdims=True)
            weight_total = totals[panel_rows:panel_rows + 1]
            pheno_total = totals[panel_rows + 1:panel_rows + 2]
            part_scales = [
                1.0 / jnp.maximum(columns[panel_rows:panel_rows + 1, i:i + 1], 1.0) for i in range(n_line)
            ]
        moment_sum = list(notes[0])
        for item in notes[1:]:
            moment_sum = [u + v for u, v in zip(moment_sum, item)]
        average = moment_sum[0] / weight_total
        second = moment_sum[1] / weight_total
        spread = 1.0 / jnp.sqrt(second - average * average + EPSILON)
        shifts = [item[0] * part_scales[i] - average for i, item in enumerate(notes)]
        shifts.append(jnp.zeros((128 - n_line, width), f32))
        correction = jnp.dot(
            columns[:panel_rows], jnp.concatenate(shifts, axis=0),
            precision=HIGHEST, preferred_element_type=f32,
        )
        unit_panel = spread * (panel_sum + correction)
        pheno_unit = spread * (moment_sum[2] - average * pheno_total)
        inverse = jnp.concatenate(inverse_parts[h * block_tiles:(h + 1) * block_tiles], axis=1)
        coef[h, 0] = (spread * unit_panel * inverse).astype(bf16)
        means[h, 0] = jnp.concatenate(
            [average[:, t * 128:(t + 1) * 128] for t in range(block_tiles)]
            + [jnp.zeros((8 - block_tiles, 128), f32)],
            axis=0,
        )
        for o in far_first:
            start(coef_copies(h, 0, (n_line - o) * PAIR, o, line_peer(o)))
        start(coef_copies(h, 0, 1, 0, partner))
        energy_snps = pheno_unit * pheno_unit * inverse
        for t in range(block_tiles):
            part = jnp.sum(energy_snps[:, t * 128:(t + 1) * 128], axis=1, keepdims=True)
            energy = energy + jnp.where(lanes == own_tiles[h * block_tiles + t], part, 0.0)

    wide_lane = lax.broadcasted_iota(jnp.int32, (1, width), 1)
    low_wide = lax.broadcasted_iota(jnp.int32, (16, width), 0)
    plan = []
    for h in range(halves):
        plan += [(h, 0, 0)] + [(h, o, 0) for o in near_first]
        if h == 0:
            plan += [(h, 0, 1)]
    for h in range(halves):
        plan += ([(h, 0, 1)] if h else []) + [(h, o, 1) for o in near_first]
    for step, (h, o, other) in enumerate(plan):
        slot = o * PAIR + other
        if slot != 0:
            received(coef_copies(h, 0, slot, 0, partner))
            if other == 0:
                start(coef_copies(h, slot, slot + 1, n_line + o, partner))
        owner = owner_of(o, other)
        comp = jnp.zeros((1, width), jnp.int32)
        for tt in range(block_tiles):
            number = tile_smem[tile_first + owner * chunk_tiles + h * block_tiles + tt]
            comp = jnp.where(lax.div(wide_lane, 128) == tt, number, comp)
        part = coef[h, slot]
        for k in range(COMPS):
            mask = (comp == k).astype(f32).astype(bf16)
            spread_coef[step % 2, k * panel_rows:(k + 1) * panel_rows, :] = part * mask
        note = means[h, slot]
        average = jnp.concatenate([note[t:t + 1] for t in range(block_tiles)], axis=1)
        high = average.astype(bf16).astype(f32)
        rest = average - high
        middle = rest.astype(bf16).astype(f32)
        dosage[h, slot, height:, :] = jnp.where(
            low_wide == 0, high, jnp.where(low_wide == 1, middle, jnp.where(low_wide == 2, rest - middle, 0.0))
        ).astype(bf16)
        product = lax.dot_general(
            dosage[h, slot], spread_coef[step % 2], (((1,), (1,)), ((), ())), preferred_element_type=f32
        )
        if step == 0:
            total[...] = product
        else:
            total[...] += product

    centre = total[height:height + 1, :] + (total[height + 1:height + 2, :] + total[height + 2:height + 3, :])
    total[:height, :] = (total[:height, :] - centre) * jnp.concatenate(
        [root_wide] * (COMPS * probe_count // 128), axis=1
    )
    for o in range(1, n_snp):
        peer = snp_peer(o)
        piece_out[o] = total[pl.ds(pl.multiple_of(peer * rows, rows), rows), :].astype(bf16)
        remote(piece_out.at[o], piece_in.at[o], send_piece.at[o], recv_piece.at[o], "snp", peer).start()
    image = total[pl.ds(pl.multiple_of(mine * rows, rows), rows), :]
    for o in range(1, n_snp):
        remote(piece_out.at[o], piece_in.at[o], send_piece.at[o], recv_piece.at[o], "snp", snp_peer(o)).wait_recv()
        image = image + piece_in[o].astype(f32)
    images_ref[...] = image.astype(bf16)

    span = COMPS * probe_count
    turned = pltpu.roll(image, span - probe_count, 1)
    sums = []
    for d in range(COMPS):
        base = image if d % 2 == 0 else turned
        cut = (d // 2) * 2 * probe_count
        other = base if cut == 0 else jnp.concatenate([base[:, cut:], base[:, :cut]], axis=1)
        sums.append(jnp.sum(image * other, axis=0, keepdims=True))
    stacked = jnp.concatenate(sums, axis=0)
    picker = (
        lax.div(lax.broadcasted_iota(jnp.int32, (span, 128), 0), probe_count)
        == lax.rem(lax.broadcasted_iota(jnp.int32, (span, 128), 1), COMPS)
    ).astype(f32)
    pairs = jnp.dot(stacked, picker, precision=HIGHEST, preferred_element_type=f32)
    row_id = lax.broadcasted_iota(jnp.int32, (COMPS, 128), 0)
    lane_id = lax.broadcasted_iota(jnp.int32, (COMPS, 128), 1)
    flat = jnp.sum(jnp.where(lax.div(lane_id, COMPS) == row_id, pairs, 0.0), axis=0, keepdims=True)
    flat = flat + pltpu.roll(jnp.broadcast_to(energy, (8, 128)), COMPS * COMPS, 1)[0:1]

    sum_samp[me] = flat
    for o in range(1, n_samp):
        remote(sum_samp.at[me], sum_samp.at[me], send_samp.at[o], recv_samp.at[o], "samp", samp_peer(o)).start()
    for o in range(1, n_samp):
        source = lax.rem(me + n_samp - o, n_samp)
        remote(sum_samp.at[source], sum_samp.at[source], send_samp.at[o], recv_samp.at[o], "samp", samp_peer(o)).wait_recv()
    group_sum = sum_samp[0]
    for i in range(1, n_samp):
        group_sum = group_sum + sum_samp[i]
    sum_mid[...] = group_sum
    for o in range(1, n_snp):
        remote(sum_mid, sum_snp.at[mine], send_snp.at[o], recv_snp.at[o], "snp", snp_peer(o)).start()
    sum_snp[mine] = group_sum
    for o in range(1, n_snp):
        source = lax.rem(mine + n_snp - o, n_snp)
        remote(sum_mid, sum_snp.at[source], send_snp.at[o], recv_snp.at[o], "snp", snp_peer(o)).wait_recv()
    everything = sum_snp[0]
    for i in range(1, n_snp):
        everything = everything + sum_snp[i]
    column_id = lax.rem(lane_id, COMPS)
    keep_lane = (lane_id < COMPS * COMPS) & (lax.div(lane_id, COMPS) == ((row_id - column_id) & (COMPS - 1)))
    chosen = jnp.where(keep_lane, jnp.broadcast_to(everything, (COMPS, 128)), 0.0)
    fold = (
        lax.rem(lax.broadcasted_iota(jnp.int32, (128, 128), 0), COMPS)
        == lax.broadcasted_iota(jnp.int32, (128, 128), 1)
    ).astype(f32)
    trace = jnp.dot(chosen, fold, precision=HIGHEST, preferred_element_type=f32)
    trace = trace * (SNPS / (COMPS * probe_count)) / (weight_total * weight_total)
    traces_ref[...] = trace[:, :COMPS]
    energies = pltpu.roll(jnp.broadcast_to(everything, (8, 128)), 128 - COMPS * COMPS, 1)[0:1]
    yky_ref[...] = (energies / weight_total)[:, :COMPS]

    sent = []
    for h in range(halves):
        for o in range(n_line):
            sent += pair_copies(h, o)
        for o in range(1, n_line):
            sent += line_copies(h, o)
            sent += coef_copies(h, 0, (n_line - o) * PAIR, o, line_peer(o))
            sent += coef_copies(h, o * PAIR, o * PAIR + 1, n_line + o, partner)
        sent += coef_copies(h, 0, 1, 0, partner)
    for o in range(1, n_samp):
        sent.append(remote(sum_samp.at[me], sum_samp.at[me], send_samp.at[o], recv_samp.at[o], "samp", samp_peer(o)))
    for o in range(1, n_snp):
        sent.append(remote(piece_out.at[o], piece_in.at[o], send_piece.at[o], recv_piece.at[o], "snp", snp_peer(o)))
        sent.append(remote(sum_mid, sum_snp.at[mine], send_snp.at[o], recv_snp.at[o], "snp", snp_peer(o)))
    for item in sent:
        item.wait_send()


def on_device_fused(geno_words, counts, probes, phenotype, tile_comp):
    n_samp, n_snp = lax.axis_size("samp"), lax.axis_size("snp")
    height = geno_words.shape[0]
    tiles_local = geno_words.shape[1] * 16 // 128
    probe_count = probes.shape[1]
    n_line = n_samp // PAIR
    halves = HALVES if tiles_local // n_samp % HALVES == 0 else 1
    block_tiles = tiles_local // n_samp // halves
    width = block_tiles * 128
    note_rows = -(-(3 * block_tiles + 1) // 8) * 8
    span = COMPS * probe_count
    rows = height // n_snp
    f32, bf16 = jnp.float32, jnp.bfloat16
    vmem = pl.BlockSpec(memory_space=pltpu.VMEM)
    smem = pl.BlockSpec(memory_space=pltpu.SMEM)
    dma = pltpu.SemaphoreType.DMA
    images, traces, yky = pl.pallas_call(
        functools.partial(whole_kernel, (n_samp, n_snp, tiles_local, probe_count, halves)),
        out_shape=(
            jax.ShapeDtypeStruct((rows, span), bf16),
            jax.ShapeDtypeStruct((COMPS, COMPS), f32),
            jax.ShapeDtypeStruct((1, COMPS), f32),
        ),
        in_specs=[smem] + [vmem] * 5,
        out_specs=(vmem, vmem, vmem),
        scratch_shapes=[
            pltpu.VMEM((halves, n_samp, height + 16, width), bf16),
            pltpu.VMEM((halves, n_line, probe_count, width), f32),
            pltpu.VMEM((halves, n_line, probe_count, width), bf16),
            pltpu.VMEM((halves, n_line, note_rows, 128), f32),
            pltpu.VMEM((halves, n_line, probe_count, width), bf16),
            pltpu.VMEM((halves, n_line, note_rows, 128), f32),
            pltpu.VMEM((halves, n_line, probe_count, width), bf16),
            pltpu.VMEM((halves, n_line, note_rows, 128), f32),
            pltpu.VMEM((halves, n_line, probe_count, width), bf16),
            pltpu.VMEM((halves, n_line, note_rows, 128), f32),
            pltpu.VMEM((halves, n_samp, probe_count, width), bf16),
            pltpu.VMEM((halves, n_samp, 8, 128), f32),
            pltpu.VMEM((2, span, width), bf16),
            pltpu.VMEM((height + 16, span), f32),
            pltpu.VMEM((n_snp, rows, span), bf16),
            pltpu.VMEM((n_snp, rows, span), bf16),
            pltpu.VMEM((n_samp, 1, 128), f32),
            pltpu.VMEM((n_snp, 1, 128), f32),
            pltpu.VMEM((1, 128), f32),
        ]
        + [dma((halves, n_line))] * 8
        + [dma((halves, n_samp))] * 4
        + [dma((n_snp,))] * 2
        + [dma((n_samp,))] * 2
        + [dma((n_snp,))] * 2,
        compiler_params=pltpu.CompilerParams(collective_id=0, has_side_effects=True),
    )(
        tile_comp,
        geno_words,
        counts.reshape(1, -1),
        probes.T,
        phenotype.reshape(1, -1),
        tile_comp.reshape(1, -1),
    )
    return (images, traces, yky.reshape(-1))


def dispatch(geno_words, counts, probes, phenotype, tile_comp):
    n_samp, n_snp = lax.axis_size("samp"), lax.axis_size("snp")
    tiles_local = geno_words.shape[1] * 16 // 128
    whole_tiles = tiles_local % n_samp == 0 and n_samp % PAIR == 0 and tile_comp.shape[0] == 128
    whole_rows = geno_words.shape[0] % (16 * n_snp) == 0 and probes.shape[1] == 64
    body = on_device_fused if whole_tiles and whole_rows else on_device
    return body(geno_words, counts, probes, phenotype, tile_comp)


def solution(mesh):
    in_specs = (P("samp", "snp"), P("samp"), P("samp", None), P("samp"), P())
    out_specs = (P(("samp", "snp"), None), P(), P())
    return jax.shard_map(
        dispatch, mesh=mesh, in_specs=in_specs, out_specs=out_specs, check_vma=False
    )
```

```python
import functools
import jax
import jax.numpy as jnp
from jax import lax
from jax.experimental import pallas as pl
from jax.experimental.pallas import tpu as pltpu
from jax.sharding import PartitionSpec as P

SNPS = 16384
COMPS = 8


EPSILON = 1e-05


def unpack_rows(packed):
    height = packed.shape[0]
    grouped = packed.reshape(height, -1, 1, 128)
    shifts = 2 * jnp.arange(16, dtype=jnp.int32).reshape(1, 1, 16, 1)
    fields = jnp.right_shift(grouped, shifts) & 3
    return fields.reshape(height, -1).astype(jnp.bfloat16)


def block_number(row_count):
    number = 1
    while row_count // number > 768 or row_count % number != 0:
        number = number + 1
    return number


def finish(panel_part, moment_part, totals, inverse, member):
    weight_total = totals[0]
    pheno_total = totals[1]
    probe_total = totals[2:]
    average = moment_part[0] / weight_total
    second = moment_part[1] / weight_total
    spread = 1.0 / jnp.sqrt(second - average * average + EPSILON)
    unit_panel = spread[:, None] * (panel_part - average[:, None] * probe_total[None, :])
    pheno_unit = spread * (moment_part[2] - average * pheno_total)
    coefficients = (spread[:, None] * unit_panel * inverse[:, None]).astype(jnp.bfloat16)
    energy = jnp.sum(member * (pheno_unit * pheno_unit * inverse)[:, None], axis=0)
    return (average, coefficients, energy)


def on_device(geno_words, counts, probes, phenotype, tile_comp):
    height = geno_words.shape[0]
    snp_local = geno_words.shape[1] * 16
    tile_local = snp_local // 128
    probe_count = probes.shape[1]
    weights = counts.astype(jnp.float32)
    root_weight = jnp.sqrt(weights)
    probe_rows = (probes.astype(jnp.float32) * root_weight[:, None]).astype(jnp.bfloat16)
    pheno_rows = (phenotype * root_weight).astype(jnp.bfloat16)
    count_rows = counts.astype(jnp.bfloat16)
    left_rows = jnp.stack([count_rows, pheno_rows], axis=1)
    dosage = unpack_rows(geno_words)
    cross_panel = jnp.einsum("rj,rb->jb", dosage, probe_rows, preferred_element_type=jnp.float32)
    linear = jnp.einsum("rc,rj->cj", left_rows, dosage, preferred_element_type=jnp.float32)
    squares = jnp.einsum("r,rj->j", count_rows, dosage * dosage, preferred_element_type=jnp.float32)
    moments = jnp.stack([linear[0], squares, linear[1]])
    totals = jnp.concatenate(
        [
            jnp.sum(weights)[None],
            jnp.sum(pheno_rows.astype(jnp.float32))[None],
            jnp.sum(probe_rows.astype(jnp.float32), axis=0),
        ]
    )
    levels = jnp.arange(COMPS, dtype=jnp.int32)
    member_all = (tile_comp[:, None] == levels[None, :]).astype(jnp.float32)
    comp_sizes = 128.0 * jnp.sum(member_all, axis=0)
    member_tiles = lax.dynamic_slice_in_dim(
        member_all, lax.axis_index("snp") * tile_local, tile_local, 0
    )
    member_snps = jnp.repeat(member_tiles, 128, axis=0)
    inverse = jnp.sum(member_snps * (1.0 / comp_sizes)[None, :], axis=1)
    summed_panel, summed_moments, totals = lax.psum(
        (cross_panel.reshape(-1, 128), moments, totals), "samp"
    )
    average, coefficients, energy = finish(
        summed_panel.reshape(snp_local, probe_count), summed_moments, totals, inverse, member_snps
    )
    energy = lax.psum(energy, "snp")
    coef_tiles = coefficients.reshape(tile_local, 128, probe_count)
    centre = jnp.sum(average.reshape(tile_local, 128, 1) * coef_tiles.astype(jnp.float32), axis=1)
    quarter = height // lax.axis_size("snp")
    inner_count = block_number(quarter * lax.axis_size("snp"))
    piece_rows = quarter * lax.axis_size("snp") // inner_count
    dosage = unpack_rows(geno_words)
    dosage = dosage.reshape(piece_rows, tile_local, 128)
    partial_value = (
        jnp.einsum("rtj,tjb->rtb", dosage, coef_tiles, preferred_element_type=jnp.float32)
        - centre[None]
    )
    grouped = jnp.einsum(
        "rtb,tk->rkb", partial_value, member_tiles, precision=lax.Precision.HIGHEST
    )
    scaled = grouped * root_weight[:, None, None]
    pieces = scaled.reshape(piece_rows, COMPS * probe_count)
    own_images = lax.psum_scatter(pieces, "snp", scatter_dimension=0, tiled=True)
    stacked = own_images.reshape(quarter, COMPS, probe_count)
    local_trace = jnp.einsum("rkb,rlb->kl", stacked, stacked, precision=lax.Precision.HIGHEST)
    trace_sum = lax.psum(local_trace, ("samp", "snp"))
    weight_total = totals[0]
    traces = trace_sum * (SNPS / (COMPS * probe_count)) / (weight_total * weight_total)
    return (own_images.astype(jnp.bfloat16), traces, energy / weight_total)


MESH = pl.DeviceIdType.MESH
HIGHEST = lax.Precision.HIGHEST
HALVES = 2
PAIR = 2


def whole_kernel(
    sizes,
    tile_smem,
    words_ref,
    counts_ref,
    probes_ref,
    pheno_ref,
    tile_ref,
    images_ref,
    traces_ref,
    yky_ref,
    dosage,
    keep,
    pair_out,
    pair_note_out,
    pair_in,
    pair_note_in,
    line_out,
    line_note_out,
    line_in,
    line_note_in,
    coef,
    means,
    spread_coef,
    total,
    piece_out,
    piece_in,
    sum_all,
    send_pair,
    recv_pair,
    send_pair_note,
    recv_pair_note,
    send_line,
    recv_line,
    send_line_note,
    recv_line_note,
    send_coef,
    recv_coef,
    send_means,
    recv_means,
    send_piece,
    recv_piece,
    send_all,
    recv_all,
):
    n_samp, n_snp, tiles_local, probe_count, halves = sizes
    me, mine = lax.axis_index("samp"), lax.axis_index("snp")
    n_line = n_samp // PAIR
    line, side = lax.div(me, PAIR), lax.rem(me, PAIR)
    partner = line * PAIR + (1 - side)
    chunk_tiles = tiles_local // n_samp
    block_tiles = chunk_tiles // halves
    width = block_tiles * 128
    note_rows = pair_note_in.shape[2]
    height = words_ref.shape[0]
    rows = height // n_snp
    panel_rows = probe_count
    f32, bf16 = jnp.float32, jnp.bfloat16

    def samp_peer(offset):
        return lax.rem(me + offset, n_samp)

    def snp_peer(offset):
        return lax.rem(mine + offset, n_snp)

    def across(offset):
        place, bit = line, 1
        while bit <= offset:
            if offset & bit:
                place = place + bit - 2 * bit * lax.rem(lax.div(line, bit), 2)
            bit = 2 * bit
        return place

    def line_peer(offset):
        return across(offset) * PAIR + side

    def owner_of(offset, other):
        return across(offset) * PAIR + (1 - side if other else side)

    half_line = n_line // 2
    far_first = list(range(half_line, n_line)) + list(range(1, half_line))
    near_first = list(range(1, half_line)) + list(reversed(range(half_line, n_line)))

    everyone = n_samp * n_snp
    spot = me * n_snp + mine

    def anyone(offset):
        other = lax.rem(spot + offset, everyone)
        return {"samp": lax.div(other, n_snp), "snp": lax.rem(other, n_snp)}

    barrier = pltpu.get_barrier_semaphore()
    for o in range(1, everyone):
        pl.semaphore_signal(barrier, inc=1, device_id=anyone(o), device_id_type=MESH)

    def sum_copy(slot, offset):
        return pltpu.make_async_remote_copy(
            src_ref=sum_all.at[slot], dst_ref=sum_all.at[slot],
            send_sem=send_all.at[offset], recv_sem=recv_all.at[offset],
            device_id=anyone(offset), device_id_type=MESH,
        )

    def remote(src, dst, send, recv, axis, peer):
        return pltpu.make_async_remote_copy(
            src_ref=src, dst_ref=dst, send_sem=send, recv_sem=recv,
            device_id={axis: peer}, device_id_type=MESH,
        )

    def pair_copies(h, o):
        return (
            remote(pair_out.at[h, o], pair_in.at[h, o], send_pair.at[h, o], recv_pair.at[h, o], "samp", partner),
            remote(pair_note_out.at[h, o], pair_note_in.at[h, o], send_pair_note.at[h, o], recv_pair_note.at[h, o], "samp", partner),
        )

    def line_copies(h, o):
        return (
            remote(line_out.at[h, o], line_in.at[h, o], send_line.at[h, o], recv_line.at[h, o], "samp", line_peer(o)),
            remote(line_note_out.at[h, o], line_note_in.at[h, o], send_line_note.at[h, o], recv_line_note.at[h, o], "samp", line_peer(o)),
        )

    def coef_copies(h, source, target, send, peer):
        return (
            remote(coef.at[h, source], coef.at[h, target], send_coef.at[h, send], recv_coef.at[h, target], "samp", peer),
            remote(means.at[h, source], means.at[h, target], send_means.at[h, send], recv_means.at[h, target], "samp", peer),
        )

    def start(copies):
        for item in copies:
            item.start()

    def received(copies):
        for item in copies:
            item.wait_recv()

    def note_of(first, second, third, last):
        parts = [v[:, t * 128:(t + 1) * 128] for v in (first, second, third) for t in range(block_tiles)]
        parts.append(last)
        spare = note_rows - len(parts)
        if spare:
            parts.append(jnp.zeros((spare, 128), f32))
        return jnp.concatenate(parts, axis=0)

    def wide_of(note, row):
        return jnp.concatenate([note[row * block_tiles + t:row * block_tiles + t + 1] for t in range(block_tiles)], axis=1)

    def last_of(note):
        return note[3 * block_tiles:3 * block_tiles + 1]

    weights = counts_ref[...].astype(f32)
    root = jnp.sqrt(weights)
    probe_rows = (probes_ref[...].astype(f32) * root).astype(bf16)
    pheno_rows = (pheno_ref[...] * root).astype(bf16)
    low = lax.broadcasted_iota(jnp.int32, (16, height), 0)
    extra = jnp.where(
        low == 0, weights, jnp.where(low == 1, pheno_rows.astype(f32), 0.0)
    ).astype(bf16)
    left = jnp.concatenate([probe_rows, extra], axis=0)
    count_left = jnp.where(low == 0, weights, 0.0).astype(bf16)

    own_sums = jnp.sum(left.astype(f32), axis=1, keepdims=True)
    own_column = own_sums[:panel_rows]
    own_weight = own_sums[panel_rows:panel_rows + 1]
    padded = jnp.concatenate(
        [
            jnp.broadcast_to(own_sums, (panel_rows + 16, 128)),
            jnp.zeros((128 - panel_rows - 16, 128), f32),
        ],
        axis=0,
    )
    own_row = padded.T[0:1]
    own_scale = 1.0 / jnp.maximum(own_weight, 1.0)

    def block(h, o, other):
        owner = owner_of(o, other)
        pieces = []
        for tt in range(block_tiles):
            tile = owner * chunk_tiles + h * block_tiles + tt
            group = lax.div(tile, 16)
            shift = 2 * lax.rem(tile, 16)
            words = words_ref[:, pl.ds(pl.multiple_of(group * 128, 128), 128)]
            field = lax.shift_right_logical(words, jnp.broadcast_to(shift, words.shape)) & 3
            pieces.append(field.astype(f32).astype(bf16))
        x = jnp.concatenate(pieces, axis=1)
        dosage[h, o * PAIR + other, :height, :] = x
        linear = jnp.dot(left, x, preferred_element_type=f32)
        squares = jnp.dot(count_left, x * x, preferred_element_type=f32)
        first = linear[panel_rows:panel_rows + 1]
        middle = first * own_scale
        panel = linear[:panel_rows] - own_column * middle
        return panel, first, squares[0:1], linear[panel_rows + 1:panel_rows + 2], middle

    waited = False
    for h in range(halves):
        for o in far_first + [0]:
            panel, first, square, cross, middle = block(h, o, 1)
            pair_out[h, o] = panel.astype(bf16)
            pair_note_out[h, o] = note_of(first, square, cross, own_row)
            if not waited:
                pl.semaphore_wait(barrier, everyone - 1)
                waited = True
            start(pair_copies(h, o))
    own_notes = {}
    for h in range(halves):
        for o in far_first + [0]:
            panel, first, square, cross, middle = block(h, o, 0)
            keep[h, o] = panel
            own_notes[h, o] = (first, square, cross, middle)
    root_wide = jnp.broadcast_to(root, (128, height)).T

    other_column = None
    own_pair = {}
    for h in range(halves):
        for o in far_first + [0]:
            received(pair_copies(h, o))
            note = pair_note_in[h, o]
            if other_column is None:
                other_row = last_of(note)
                turned = jnp.broadcast_to(other_row, (128, 128)).T[:, 0:1]
                other_column = turned[:panel_rows]
                other_weight = turned[panel_rows:panel_rows + 1]
                other_scale = 1.0 / jnp.maximum(other_weight, 1.0)
                pair_scale = 1.0 / jnp.maximum(own_weight + other_weight, 1.0)
                pair_row = own_row + other_row
            first, square, cross, middle = own_notes[h, o]
            other_first = wide_of(note, 0)
            pair_first = first + other_first
            pair_middle = pair_first * pair_scale
            panel = (
                keep[h, o]
                + pair_in[h, o].astype(f32)
                + own_column * (middle - pair_middle)
                + other_column * (other_first * other_scale - pair_middle)
            )
            pair_note = (pair_first, square + wide_of(note, 1), cross + wide_of(note, 2))
            if o == 0:
                own_pair[h] = (panel, pair_note)
            else:
                line_out[h, o] = panel.astype(bf16)
                line_note_out[h, o] = note_of(*pair_note, pair_row)
                start(line_copies(h, o))

    tile_all = tile_ref[...]
    lanes = lax.broadcasted_iota(jnp.int32, (1, 128), 1)
    tile_first = mine * tiles_local
    own_tiles = [tile_smem[tile_first + me * chunk_tiles + tt] for tt in range(chunk_tiles)]
    inverse_parts = []
    for tt in range(chunk_tiles):
        size = 128.0 * jnp.sum((tile_all == own_tiles[tt]).astype(f32), axis=1, keepdims=True)
        inverse_parts.append(jnp.broadcast_to(1.0 / size, (1, 128)))

    columns = None
    energy = jnp.zeros((1, 128), f32)
    for h in range(halves):
        panel_sum, own_note = own_pair[h]
        notes = [own_note]
        last_rows = [pair_row]
        for o in far_first:
            received(line_copies(h, o))
            note = line_note_in[h, o]
            panel_sum = panel_sum + line_in[h, o].astype(f32)
            notes.append((wide_of(note, 0), wide_of(note, 1), wide_of(note, 2)))
            last_rows.append(last_of(note))
        if columns is None:
            columns = jnp.concatenate(last_rows + [jnp.zeros((128 - n_line, 128), f32)], axis=0).T
            totals = jnp.sum(columns, axis=1, keepdims=True)
            weight_total = totals[panel_rows:panel_rows + 1]
            pheno_total = totals[panel_rows + 1:panel_rows + 2]
            part_scales = [
                1.0 / jnp.maximum(columns[panel_rows:panel_rows + 1, i:i + 1], 1.0) for i in range(n_line)
            ]
        moment_sum = list(notes[0])
        for item in notes[1:]:
            moment_sum = [u + v for u, v in zip(moment_sum, item)]
        average = moment_sum[0] / weight_total
        second = moment_sum[1] / weight_total
        spread = 1.0 / jnp.sqrt(second - average * average + EPSILON)
        shifts = [item[0] * part_scales[i] - average for i, item in enumerate(notes)]
        shifts.append(jnp.zeros((128 - n_line, width), f32))
        correction = jnp.dot(
            columns[:panel_rows], jnp.concatenate(shifts, axis=0),
            precision=HIGHEST, preferred_element_type=f32,
        )
        unit_panel = spread * (panel_sum + correction)
        pheno_unit = spread * (moment_sum[2] - average * pheno_total)
        inverse = jnp.concatenate(inverse_parts[h * block_tiles:(h + 1) * block_tiles], axis=1)
        coef[h, 0] = (spread * unit_panel * inverse).astype(bf16)
        means[h, 0] = jnp.concatenate(
            [average[:, t * 128:(t + 1) * 128] for t in range(block_tiles)]
            + [jnp.zeros((8 - block_tiles, 128), f32)],
            axis=0,
        )
        for o in far_first:
            start(coef_copies(h, 0, o * PAIR, o, line_peer(o)))
        start(coef_copies(h, 0, 1, 0, partner))
        energy_snps = pheno_unit * pheno_unit * inverse
        for t in range(block_tiles):
            part = jnp.sum(energy_snps[:, t * 128:(t + 1) * 128], axis=1, keepdims=True)
            energy = energy + jnp.where(lanes == own_tiles[h * block_tiles + t], part, 0.0)

    wide_lane = lax.broadcasted_iota(jnp.int32, (1, width), 1)
    low_wide = lax.broadcasted_iota(jnp.int32, (16, width), 0)
    plan = []
    for h in range(halves):
        plan += [(h, 0, 0)] + [(h, o, 0) for o in near_first]
        if h == 0:
            plan += [(h, 0, 1)]
    for h in range(halves):
        plan += ([(h, 0, 1)] if h else []) + [(h, o, 1) for o in near_first]
    for step, (h, o, other) in enumerate(plan):
        slot = o * PAIR + other
        if slot != 0:
            received(coef_copies(h, 0, slot, 0, partner))
            if other == 0:
                start(coef_copies(h, slot, slot + 1, n_line + o, partner))
        owner = owner_of(o, other)
        comp = jnp.zeros((1, width), jnp.int32)
        for tt in range(block_tiles):
            number = tile_smem[tile_first + owner * chunk_tiles + h * block_tiles + tt]
            comp = jnp.where(lax.div(wide_lane, 128) == tt, number, comp)
        part = coef[h, slot]
        for k in range(COMPS):
            mask = (comp == k).astype(f32).astype(bf16)
            spread_coef[step % 2, k * panel_rows:(k + 1) * panel_rows, :] = part * mask
        note = means[h, slot]
        average = jnp.concatenate([note[t:t + 1] for t in range(block_tiles)], axis=1)
        high = average.astype(bf16).astype(f32)
        rest = average - high
        middle = rest.astype(bf16).astype(f32)
        dosage[h, slot, height:, :] = jnp.where(
            low_wide == 0, high, jnp.where(low_wide == 1, middle, jnp.where(low_wide == 2, rest - middle, 0.0))
        ).astype(bf16)
        product = lax.dot_general(
            dosage[h, slot], spread_coef[step % 2], (((1,), (1,)), ((), ())), preferred_element_type=f32
        )
        if step == 0:
            total[...] = product
        else:
            total[...] += product

    centre = total[height:height + 1, :] + (total[height + 1:height + 2, :] + total[height + 2:height + 3, :])
    total[:height, :] = (total[:height, :] - centre) * jnp.concatenate(
        [root_wide] * (COMPS * probe_count // 128), axis=1
    )
    for o in range(1, n_snp):
        peer = snp_peer(o)
        piece_out[o] = total[pl.ds(pl.multiple_of(peer * rows, rows), rows), :].astype(bf16)
        remote(piece_out.at[o], piece_in.at[o], send_piece.at[o], recv_piece.at[o], "snp", peer).start()
    image = total[pl.ds(pl.multiple_of(mine * rows, rows), rows), :]
    for o in range(1, n_snp):
        remote(piece_out.at[o], piece_in.at[o], send_piece.at[o], recv_piece.at[o], "snp", snp_peer(o)).wait_recv()
        image = image + piece_in[o].astype(f32)
    images_ref[...] = image.astype(bf16)

    span = COMPS * probe_count
    turned = pltpu.roll(image, span - probe_count, 1)
    sums = []
    for d in range(COMPS):
        base = image if d % 2 == 0 else turned
        cut = (d // 2) * 2 * probe_count
        other = base if cut == 0 else jnp.concatenate([base[:, cut:], base[:, :cut]], axis=1)
        sums.append(jnp.sum(image * other, axis=0, keepdims=True))
    stacked = jnp.concatenate(sums, axis=0)
    picker = (
        lax.div(lax.broadcasted_iota(jnp.int32, (span, 128), 0), probe_count)
        == lax.rem(lax.broadcasted_iota(jnp.int32, (span, 128), 1), COMPS)
    ).astype(f32)
    pairs = jnp.dot(stacked, picker, precision=HIGHEST, preferred_element_type=f32)
    row_id = lax.broadcasted_iota(jnp.int32, (COMPS, 128), 0)
    lane_id = lax.broadcasted_iota(jnp.int32, (COMPS, 128), 1)
    flat = jnp.sum(jnp.where(lax.div(lane_id, COMPS) == row_id, pairs, 0.0), axis=0, keepdims=True)
    flat = flat + pltpu.roll(jnp.broadcast_to(energy, (8, 128)), COMPS * COMPS, 1)[0:1]

    sum_all[spot] = flat
    for o in range(1, everyone):
        sum_copy(spot, o).start()
    for o in range(1, everyone):
        sum_copy(lax.rem(spot + everyone - o, everyone), o).wait_recv()
    everything = jnp.sum(sum_all[...], axis=0)
    column_id = lax.rem(lane_id, COMPS)
    keep_lane = (lane_id < COMPS * COMPS) & (lax.div(lane_id, COMPS) == ((row_id - column_id) & (COMPS - 1)))
    chosen = jnp.where(keep_lane, jnp.broadcast_to(everything, (COMPS, 128)), 0.0)
    fold = (
        lax.rem(lax.broadcasted_iota(jnp.int32, (128, 128), 0), COMPS)
        == lax.broadcasted_iota(jnp.int32, (128, 128), 1)
    ).astype(f32)
    trace = jnp.dot(chosen, fold, precision=HIGHEST, preferred_element_type=f32)
    trace = trace * (SNPS / (COMPS * probe_count)) / (weight_total * weight_total)
    traces_ref[...] = trace[:, :COMPS]
    energies = pltpu.roll(jnp.broadcast_to(everything, (8, 128)), 128 - COMPS * COMPS, 1)[0:1]
    yky_ref[...] = (energies / weight_total)[:, :COMPS]

    sent = []
    for h in range(halves):
        for o in range(n_line):
            sent += pair_copies(h, o)
        for o in range(1, n_line):
            sent += line_copies(h, o)
            sent += coef_copies(h, 0, o * PAIR, o, line_peer(o))
            sent += coef_copies(h, o * PAIR, o * PAIR + 1, n_line + o, partner)
        sent += coef_copies(h, 0, 1, 0, partner)
    for o in range(1, everyone):
        sent.append(sum_copy(spot, o))
    for o in range(1, n_snp):
        sent.append(remote(piece_out.at[o], piece_in.at[o], send_piece.at[o], recv_piece.at[o], "snp", snp_peer(o)))
    for item in sent:
        item.wait_send()


def hand_over(images_in, traces_in, yky_in, images_ref, traces_ref, yky_ref):
    images_ref[...] = images_in[...]
    traces_ref[...] = traces_in[...]
    yky_ref[...] = yky_in[...]


def on_device_fused(geno_words, counts, probes, phenotype, tile_comp):
    n_samp, n_snp = lax.axis_size("samp"), lax.axis_size("snp")
    height = geno_words.shape[0]
    tiles_local = geno_words.shape[1] * 16 // 128
    probe_count = probes.shape[1]
    n_line = n_samp // PAIR
    halves = HALVES if tiles_local // n_samp % HALVES == 0 else 1
    block_tiles = tiles_local // n_samp // halves
    width = block_tiles * 128
    note_rows = -(-(3 * block_tiles + 1) // 8) * 8
    span = COMPS * probe_count
    rows = height // n_snp
    f32, bf16 = jnp.float32, jnp.bfloat16
    vmem = pl.BlockSpec(memory_space=pltpu.VMEM)
    smem = pl.BlockSpec(memory_space=pltpu.SMEM)
    dma = pltpu.SemaphoreType.DMA
    images, traces, yky = pl.pallas_call(
        functools.partial(whole_kernel, (n_samp, n_snp, tiles_local, probe_count, halves)),
        out_shape=(
            jax.ShapeDtypeStruct((rows, span), bf16),
            jax.ShapeDtypeStruct((COMPS, COMPS), f32),
            jax.ShapeDtypeStruct((1, COMPS), f32),
        ),
        in_specs=[smem] + [vmem] * 5,
        out_specs=(vmem, vmem, vmem),
        scratch_shapes=[
            pltpu.VMEM((halves, n_samp, height + 16, width), bf16),
            pltpu.VMEM((halves, n_line, probe_count, width), f32),
            pltpu.VMEM((halves, n_line, probe_count, width), bf16),
            pltpu.VMEM((halves, n_line, note_rows, 128), f32),
            pltpu.VMEM((halves, n_line, probe_count, width), bf16),
            pltpu.VMEM((halves, n_line, note_rows, 128), f32),
            pltpu.VMEM((halves, n_line, probe_count, width), bf16),
            pltpu.VMEM((halves, n_line, note_rows, 128), f32),
            pltpu.VMEM((halves, n_line, probe_count, width), bf16),
            pltpu.VMEM((halves, n_line, note_rows, 128), f32),
            pltpu.VMEM((halves, n_samp, probe_count, width), bf16),
            pltpu.VMEM((halves, n_samp, 8, 128), f32),
            pltpu.VMEM((2, span, width), bf16),
            pltpu.VMEM((height + 16, span), f32),
            pltpu.VMEM((n_snp, rows, span), bf16),
            pltpu.VMEM((n_snp, rows, span), bf16),
            pltpu.VMEM((n_samp * n_snp, 1, 128), f32),
        ]
        + [dma((halves, n_line))] * 8
        + [dma((halves, n_samp))] * 4
        + [dma((n_snp,))] * 2
        + [dma((n_samp * n_snp,))] * 2,
        compiler_params=pltpu.CompilerParams(collective_id=0, has_side_effects=True),
    )(
        tile_comp,
        geno_words,
        counts.reshape(1, -1),
        probes.T,
        phenotype.reshape(1, -1),
        tile_comp.reshape(1, -1),
    )
    images, traces, yky = pl.pallas_call(
        hand_over,
        out_shape=tuple(jax.ShapeDtypeStruct(v.shape, v.dtype) for v in (images, traces, yky)),
        in_specs=[vmem] * 3,
        out_specs=(vmem, vmem, vmem),
    )(images, traces, yky)
    return (images, traces, yky.reshape(-1))


def dispatch(geno_words, counts, probes, phenotype, tile_comp):
    n_samp, n_snp = lax.axis_size("samp"), lax.axis_size("snp")
    tiles_local = geno_words.shape[1] * 16 // 128
    whole_tiles = tiles_local % n_samp == 0 and n_samp % PAIR == 0 and (n_samp // PAIR) & (n_samp // PAIR - 1) == 0 and tile_comp.shape[0] == 128
    whole_rows = geno_words.shape[0] % (16 * n_snp) == 0 and probes.shape[1] == 64
    body = on_device_fused if whole_tiles and whole_rows else on_device
    return body(geno_words, counts, probes, phenotype, tile_comp)


def solution(mesh):
    in_specs = (P("samp", "snp"), P("samp"), P("samp", None), P("samp"), P())
    out_specs = (P(("samp", "snp"), None), P(), P())
    return jax.shard_map(
        dispatch, mesh=mesh, in_specs=in_specs, out_specs=out_specs, check_vma=False
    )
```
